32 devices in a mesh: gy: 8 (over y, x, core), gx: 4 (over z).
Axes of the slice: x: 2, y: 2, z: 4, core: 2. Of those that a mesh axis runs over, the one named last changes fastest.
Arguments:
- tracer: float32 [8, 1024, 1024], P(None, 'gy', 'gx'), may hold values from -6 to 6
- east_speed: float32 [8, 1024, 1024], P(None, 'gy', 'gx'), may hold values from -0.25 to 0.25
- north_speed: float32 [8, 1024, 1024], P(None, 'gy', 'gx'), may hold values from -0.25 to 0.25
- columns: int32 [1024, 1024], P('gy', 'gx'), may hold values from 0 to 8
- thickness: float32 [8], replicated, may hold values from 0.5 to 2
- surface_flux: float32 [1024, 1024], P('gy', 'gx'), may hold values from -6 to 6
- helm: float32 [1024, 1024], P('gy', 'gx'), may hold values from 0.2 to 4
Outputs:
- tracer_new: float32 [8, 1024, 1024], P(None, 'gy', 'gx')
- heights: float32 [1024, 1024], P('gy', 'gx')
The draws below stay inside these ranges and needn't reach their ends.
Inputs may be any that keep to these rules, and one draw needn't show every extreme that they name: `columns`: ocean levels per column; 0 means land.
All inputs are finite; a program needn't handle non-finite values.
Results may differ from the reference program's by a relative error of at most 0.0001.
Values sent between devices are 32-bit elements; how exact they have to be, the bound alone decides.
A program may use at most 64 MiB of HBM per device.

```python
import math
import jax
import jax.numpy as jnp
from jax import lax

K = 8
TSTEPS = 2
ITERS = 3
NY = 1024
NX = 1024


def plant(entries, own_key, smallest, top_value):
    shape = entries.shape
    index_at = [jax.random.randint(jax.random.fold_in(own_key, axis), (), 0, shape[axis]) for axis in range(len(shape))]
    entries = entries.at[tuple(index_at)].set(smallest)
    longest = shape.index(max(shape))
    index_at[longest] = (index_at[longest] + 1) % shape[longest]
    return entries.at[tuple(index_at)].set(top_value)


def block_levels(stream_key, shape, split, least, top_value):
    def one(dim, blocks):
        steps = jax.random.uniform(jax.random.fold_in(jax.random.fold_in(stream_key, 6), dim), (blocks,), jnp.float32, least / len(split), top_value / len(split))
        return jnp.repeat(jnp.exp(steps), shape[dim] // blocks).reshape((-1,) + (1,) * (len(shape) - dim - 1))

    loudness = one(*split[0])
    for cut in split[1:]:
        loudness = loudness * one(*cut)
    return loudness


def normal_values(own_key, extent, width, bound, pieces=(), kind=jnp.bfloat16):
    drawn = width * jax.random.normal(own_key, extent, jnp.float32)
    if pieces:
        drawn = drawn * block_levels(own_key, extent, pieces, -0.22, 0.18)
    return jnp.clip(drawn, -bound, bound).astype(kind)


def setup_inputs(seed: int = 0) -> dict:
    arg_keys = jax.random.split(jax.random.key(seed), 8)
    return {
        "tracer": normal_values(arg_keys[0], (K, NY, NX), 1.0, 6.0, ((1, 8), (2, 4)), jnp.float32),
        "east_speed": jnp.clip(jax.random.uniform(arg_keys[1], (K, NY, NX), jnp.float32, -0.25, 0.25) * block_levels(arg_keys[1], (K, NY, NX), ((1, 8), (2, 4)), -0.4, 0.0), -0.25, 0.25),
        "north_speed": jnp.clip(jax.random.uniform(arg_keys[2], (K, NY, NX), jnp.float32, -0.25, 0.25) * block_levels(arg_keys[2], (K, NY, NX), ((1, 8), (2, 4)), -0.4, 0.0), -0.25, 0.25),
        "columns": plant(jax.random.randint(arg_keys[3], (NY, NX), 0, K + 1), jax.random.fold_in(arg_keys[3], 1), 0, K).astype(jnp.int32),
        "thickness": jnp.clip(jnp.exp(jax.random.uniform(arg_keys[4], (K,), jnp.float32, math.log(0.5), math.log(2.0))), 0.5, 2.0),
        "surface_flux": normal_values(arg_keys[5], (NY, NX), 1.0, 6.0, ((0, 8), (1, 4)), jnp.float32),
        "helm": jnp.clip(jnp.exp(math.log(4.0) - 2.9957323 * jax.random.uniform(arg_keys[6], (NY, NX), jnp.float32) ** block_levels(arg_keys[6], (NY, NX), ((0, 8), (1, 4)), -0.2, 0.2)), 0.2, 4.0),
    }


def upwind(speed, behind, ahead):
    return jnp.maximum(speed, 0.0) * behind + jnp.minimum(speed, 0.0) * ahead


def advect(current, east_speed, north_speed, ocean):
    tracer_east = jnp.roll(current, -1, axis=2)
    ocean_east = jnp.roll(ocean, -1, axis=2)
    tracer_north = jnp.pad(current[:, 1:, :], ((0, 0), (0, 1), (0, 0)))
    ocean_north = jnp.pad(ocean[:, 1:, :], ((0, 0), (0, 1), (0, 0)))
    flux_east = ocean * ocean_east * upwind(east_speed, current, tracer_east)
    flux_north = ocean * ocean_north * upwind(north_speed, current, tracer_north)
    flux_west = jnp.roll(flux_east, 1, axis=2)
    flux_south = jnp.pad(flux_north[:, :-1, :], ((0, 0), (1, 0), (0, 0)))
    return current - (flux_east - flux_west + flux_north - flux_south)


def neighbour(source, row_step, col_step):
    moved = jnp.roll(source, -col_step, axis=1)
    if row_step == 1:
        moved = jnp.pad(moved[1:], ((0, 1), (0, 0)))
    elif row_step == -1:
        moved = jnp.pad(moved[:-1], ((1, 0), (0, 0)))
    return moved


def nine_point(source, wet, diagonal_term):
    weighted = wet * source
    edges = neighbour(weighted, 0, 1) + neighbour(weighted, 0, -1) + neighbour(weighted, 1, 0) + neighbour(weighted, -1, 0)
    corners = neighbour(weighted, 1, 1) + neighbour(weighted, 1, -1) + neighbour(weighted, -1, 1) + neighbour(weighted, -1, -1)
    return diagonal_term * source - wet * (edges + 0.5 * corners)


def reference(tracer, east_speed, north_speed, columns, thickness, surface_flux, helm):
    depth = lax.broadcasted_iota(jnp.int32, tracer.shape, 0)
    ocean = (depth < columns[None]).astype(jnp.float32)
    current = tracer
    for section_index in range(TSTEPS):
        current = advect(current, east_speed, north_speed, ocean)
    forcing = surface_flux + jnp.sum(thickness[:, None, None] * ocean * current, axis=0)
    wet = ocean[0]
    diagonal_term = 6.0 + helm
    heights = jnp.zeros_like(forcing)
    residual = forcing
    scaled = residual / diagonal_term
    direction = scaled
    product_now = jnp.sum(residual * scaled)
    for iteration in range(ITERS):
        applied = nine_point(direction, wet, diagonal_term)
        step_size = product_now / jnp.sum(direction * applied)
        heights = heights + step_size * direction
        residual = residual - step_size * applied
        scaled = residual / diagonal_term
        product_next = jnp.sum(residual * scaled)
        direction = scaled + (product_next / product_now) * direction
        product_now = product_next
    return current, heights
```

```python
import functools

import jax
import jax.numpy as jnp
from jax import lax
from jax.experimental import pallas as pl
from jax.experimental.pallas import tpu as pltpu
from jax.sharding import PartitionSpec as P

TSTEPS = 2
ITERS = 3
MESH = pl.DeviceIdType.MESH
SUB = 8
LANE = 128
AROUND = ((1, 0), (-1, 0), (0, 1), (0, -1), (1, 1), (1, -1), (-1, 1), (-1, -1))


def roll(array, shift, axis):
    shift = shift % array.shape[axis]
    return pltpu.roll(array, shift, axis) if shift else array


def iota(shape, dim):
    return lax.broadcasted_iota(jnp.int32, shape, dim)


def kernel(
    ny,
    nx,
    tracer_ref,
    east_ref,
    north_ref,
    columns_ref,
    thickness_ref,
    surface_ref,
    helm_ref,
    tracer_out,
    heights_out,
    c_ext,
    e_ext,
    n_ext,
    col_in,
    surf_in,
    flat_ext,
    pack,
    pack_recv,
    corner_recv,
    up_send,
    down_send,
    up_recv,
    down_recv,
    forcing,
    start_vec,
    flat_pack,
    edge_pack,
    row_recv,
    edge_recv,
    edge_corner_recv,
    part,
    slots,
    in_sem,
    out_sem,
    send_sem,
    recv_sem,
    sum_send_sem,
    sum_recv_sem,
):
    levels, rows, cols = tracer_ref.shape
    ext_rows, ext_cols = rows + SUB, cols + LANE
    my_y, my_x = lax.axis_index("gy"), lax.axis_index("gx")
    count = ny * nx
    my_id = my_y * nx + my_x

    def place(offset):
        target = lax.rem(my_id + offset, count)
        return (target // nx, lax.rem(target, nx))

    def near(dy, dx):
        return (lax.rem(my_y + dy + ny, ny), lax.rem(my_x + dx + nx, nx))

    loads = [
        pltpu.make_async_copy(columns_ref, col_in, in_sem.at[0]),
        pltpu.make_async_copy(helm_ref, flat_ext.at[1, 0:rows, 0:cols], in_sem.at[1]),
        pltpu.make_async_copy(tracer_ref, c_ext.at[:, 0:rows, 0:cols], in_sem.at[2]),
        pltpu.make_async_copy(east_ref, e_ext.at[:, 0:rows, 0:cols], in_sem.at[3]),
        pltpu.make_async_copy(north_ref, n_ext.at[:, 0:rows, 0:cols], in_sem.at[4]),
        pltpu.make_async_copy(surface_ref, surf_in, in_sem.at[5]),
    ]
    for load in loads:
        load.start()
    barrier = pltpu.get_barrier_semaphore()
    for offset in range(1, count):
        pl.semaphore_signal(barrier, inc=1, device_id=place(offset), device_id_type=MESH)
    for load in loads:
        load.wait()

    fields = (c_ext, e_ext, n_ext)
    flat_ext[0, 0:rows, 0:cols] = col_in[...].astype(jnp.float32)

    lane_full = iota((rows, LANE), 1)
    lane_half = lane_full < LANE // 2
    group = ((lane_full + 2) % LANE) // 4

    def both_edges(ref, index):
        return jnp.where(lane_half, ref[index, 0:rows, 0:LANE], ref[index, 0:rows, cols - LANE : cols])

    sources = [(fields[f], k, f) for k in range(levels) for f in range(3)]
    sources += [(flat_ext, 0, 3), (flat_ext, 1, 4)]
    packed = jnp.zeros((rows, LANE), jnp.float32)
    for slot, (ref, index, _) in enumerate(sources):
        packed = jnp.where(group == slot, roll(both_edges(ref, index), 4 * slot, 1), packed)
    pack[...] = packed

    sub = iota((SUB, cols), 0)
    for k in range(levels):
        quads = [(ref, k) for ref in fields] + [(flat_ext, min(k, 1))]
        up = jnp.zeros((SUB, cols), jnp.float32)
        down = jnp.zeros((SUB, cols), jnp.float32)
        for f, (ref, index) in enumerate(quads):
            mine = sub // 2 == f
            up = jnp.where(mine, roll(ref[index, rows - SUB : rows, 0:cols], 2 * f + 2, 0), up)
            down = jnp.where(mine, roll(ref[index, 0:SUB, 0:cols], 2 * f, 0), down)
        up_send[k] = up
        down_send[k] = down

    pl.semaphore_wait(barrier, count - 1)

    first_rows, last_rows = pl.ds(0, SUB), pl.ds(rows - SUB, SUB)
    first = [
        (up_send, up_recv),
        (down_send, down_recv),
        (pack, pack_recv.at[0]),
        (pack, pack_recv.at[1]),
        (pack.at[last_rows], corner_recv.at[0]),
        (pack.at[last_rows], corner_recv.at[1]),
        (pack.at[first_rows], corner_recv.at[2]),
        (pack.at[first_rows], corner_recv.at[3]),
    ]

    def exchange(pairs, base):
        copies = []
        for which, (source, target) in enumerate(pairs):
            copies.append(
                pltpu.make_async_remote_copy(
                    src_ref=source,
                    dst_ref=target,
                    send_sem=send_sem.at[base + which],
                    recv_sem=recv_sem.at[base + which],
                    device_id=near(*AROUND[which]),
                    device_id_type=MESH,
                )
            )
        for copy in copies:
            copy.start()
        return copies

    copies = exchange(first, 0)
    for copy in copies:
        copy.wait_recv()

    from_right = (iota((rows, LANE), 1) % 4) < 2
    sides = jnp.where(from_right, pack_recv[1], pack_recv[0])
    small_right = (iota((SUB, LANE), 1) % 4) < 2
    small_below = iota((SUB, LANE), 0) < SUB // 2
    south = jnp.where(small_right, corner_recv[1], corner_recv[0])
    north = jnp.where(small_right, corner_recv[3], corner_recv[2])
    corner = jnp.where(small_below, north, south)
    for slot, (ref, index, _) in enumerate(sources):
        ref[index, 0:rows, cols:ext_cols] = roll(sides, -4 * slot, 1)
        ref[index, rows:ext_rows, cols:ext_cols] = roll(corner, -4 * slot, 1)
    for k in range(levels):
        quads = [(ref, k) for ref in fields] + ([(flat_ext, k)] if k < 2 else [])
        for f, (ref, index) in enumerate(quads):
            ref[index, rows:ext_rows, 0:cols] = jnp.where(
                sub < SUB // 2,
                roll(down_recv[k], -2 * f, 0),
                roll(up_recv[k], -2 * f - 2, 0),
            )

    row_ids = iota((SUB, ext_cols), 0)
    beyond = (row_ids >= SUB // 2) & (my_y == 0) | (row_ids < SUB // 2) & (my_y == ny - 1)
    flat_ext[0, rows:ext_rows] = jnp.where(beyond, 0.0, flat_ext[0, rows:ext_rows])

    forcing[...] = surf_in[...]

    def level(k, carry):
        depth = flat_ext[0]
        ocean = jnp.where(depth > lax.convert_element_type(k, jnp.float32), 1.0, 0.0)
        east = e_ext[k] * (ocean * roll(ocean, -1, 1))
        nort = n_ext[k] * (ocean * roll(ocean, -1, 0))
        current = c_ext[k]
        for _ in range(TSTEPS):
            flux_east = jnp.maximum(east, 0.0) * current + jnp.minimum(east, 0.0) * roll(
                current, -1, 1
            )
            flux_north = jnp.maximum(nort, 0.0) * current + jnp.minimum(nort, 0.0) * roll(
                current, -1, 0
            )
            current = current - (
                flux_east - roll(flux_east, 1, 1) + flux_north - roll(flux_north, 1, 0)
            )
        c_ext[k] = current
        forcing[...] += (thickness_ref[k] * ocean * current)[0:rows, 0:cols]
        return carry

    lax.fori_loop(0, levels, level, 0)

    out_copy = pltpu.make_async_copy(c_ext.at[:, 0:rows, 0:cols], tracer_out, out_sem)
    out_copy.start()

    diagonal = 6.0 + flat_ext[1, 0:rows, 0:cols]
    wet = jnp.where(flat_ext[0, 0:rows, 0:cols] > 0.0, 1.0, 0.0)
    z0 = forcing[...] / diagonal
    y0 = wet * z0
    start_vec[0:rows, 0:cols] = y0
    edges = jnp.where(lane_half, y0[:, 0:LANE], y0[:, cols - LANE : cols])
    flat_pack[...] = edges
    edge_pack[...] = edges.T
    last_lanes = pl.ds(LANE - SUB, SUB)
    second = [
        (start_vec.at[last_rows, pl.ds(0, cols)], row_recv.at[0]),
        (start_vec.at[first_rows, pl.ds(0, cols)], row_recv.at[1]),
        (edge_pack.at[last_lanes], edge_recv.at[0]),
        (edge_pack.at[first_rows], edge_recv.at[1]),
        (flat_pack.at[last_rows], edge_corner_recv.at[0]),
        (flat_pack.at[last_rows], edge_corner_recv.at[1]),
        (flat_pack.at[first_rows], edge_corner_recv.at[2]),
        (flat_pack.at[first_rows], edge_corner_recv.at[3]),
    ]
    more = exchange(second, len(AROUND))
    for copy in more:
        copy.wait_recv()

    turned = jnp.concatenate(
        [edge_recv[1], jnp.zeros((LANE - 2 * SUB, rows), jnp.float32), edge_recv[0]], axis=0
    )
    lane_small = iota((SUB, LANE), 1) < LANE // 2
    south = jnp.where(lane_small, edge_corner_recv[1], edge_corner_recv[0])
    north = jnp.where(lane_small, edge_corner_recv[3], edge_corner_recv[2])
    for copy in more:
        copy.wait_send()
    start_vec[0:rows, cols:ext_cols] = turned.T
    start_vec[rows:ext_rows, cols:ext_cols] = jnp.where(small_below, north, south)
    start_vec[rows:ext_rows, 0:cols] = jnp.where(sub < SUB // 2, row_recv[1], row_recv[0])
    start_vec[rows:ext_rows] = jnp.where(beyond, 0.0, start_vec[rows:ext_rows])

    scale = jnp.where(flat_ext[0] > 0.0, 1.0 / (6.0 + flat_ext[1]), 0.0)

    def off_diagonal(vector):
        across = roll(vector, 1, 1) + roll(vector, -1, 1)
        mixed = vector + 0.5 * across
        return scale * (across + roll(mixed, 1, 0) + roll(mixed, -1, 0))

    z1_ext = off_diagonal(start_vec[...])
    z2_ext = off_diagonal(z1_ext)
    z3_ext = off_diagonal(z2_ext)
    z1, z2, z3 = (z[0:rows, 0:cols] for z in (z1_ext, z2_ext, z3_ext))

    def partial(values):
        folded = jnp.sum(values, axis=0, keepdims=True)
        return sum(folded[:, i : i + LANE] for i in range(0, cols, LANE))

    d0, d1, d2 = (diagonal * z for z in (z0, z1, z2))
    sums = [partial(v) for v in (d0 * z0, d0 * z1, d1 * z1, d1 * z2, d2 * z2, d2 * z3)]
    part[...] = jnp.concatenate(sums + [jnp.zeros((SUB - len(sums), LANE), jnp.float32)], axis=0)

    for offset in range(1, count):
        pltpu.make_async_remote_copy(
            src_ref=part,
            dst_ref=slots.at[offset - 1],
            send_sem=sum_send_sem,
            recv_sem=sum_recv_sem,
            device_id=place(offset),
            device_id_type=MESH,
        ).start()
    everything = pltpu.make_async_remote_copy(
        src_ref=slots,
        dst_ref=slots,
        send_sem=sum_send_sem,
        recv_sem=sum_recv_sem,
        device_id=place(1),
        device_id_type=MESH,
    )
    everything.wait_recv()
    total = jnp.sum(jnp.sum(slots[...], axis=0) + part[...], axis=1, keepdims=True)
    moment = [total[i : i + 1, :] for i in range(2 * ITERS)]

    def inner(a, b):
        return sum(x * y * moment[i + j] for i, x in enumerate(a) for j, y in enumerate(b))

    def ratio(top, bottom):
        good = bottom > 0.0
        return jnp.where(good, top / jnp.where(good, bottom, 1.0), 0.0)

    one, zero = jnp.ones((1, 1), jnp.float32), jnp.zeros((1, 1), jnp.float32)
    scaled, direction, height = [one], [one], [zero] * ITERS
    product_now = moment[0]
    for iteration in range(ITERS):
        low, high = direction + [zero], [zero] + direction
        applied = [a - b for a, b in zip(low, high)]
        step_size = ratio(product_now, inner(direction, applied))
        for i, x in enumerate(direction):
            height[i] = height[i] + step_size * x
        if iteration + 1 < ITERS:
            scaled = [a - step_size * b for a, b in zip(scaled + [zero], applied)]
            product_next = jnp.maximum(inner(scaled, scaled), 0.0)
            factor = ratio(product_next, product_now)
            direction = [a + factor * b for a, b in zip(scaled, low)]
            product_now = product_next
    heights_out[...] = height[0] * z0 + height[1] * z1 + height[2] * z2

    everything.wait_send()
    for copy in copies:
        copy.wait_send()
    out_copy.wait()


def on_device(ny, nx, tracer, east_speed, north_speed, columns, thickness, surface_flux, helm):
    levels, rows, cols = tracer.shape
    ext = (rows + SUB, cols + LANE)
    hbm = pl.BlockSpec(memory_space=pl.ANY)
    vmem = pl.BlockSpec(memory_space=pltpu.VMEM)
    smem = pl.BlockSpec(memory_space=pltpu.SMEM)
    f32 = jnp.float32
    dma = pltpu.SemaphoreType.DMA
    scratch = [
        pltpu.VMEM((levels, *ext), f32),
        pltpu.VMEM((levels, *ext), f32),
        pltpu.VMEM((levels, *ext), f32),
        pltpu.VMEM((rows, cols), jnp.int32),
        pltpu.VMEM((rows, cols), f32),
        pltpu.VMEM((2, *ext), f32),
        pltpu.VMEM((rows, LANE), f32),
        pltpu.VMEM((2, rows, LANE), f32),
        pltpu.VMEM((4, SUB, LANE), f32),
        pltpu.VMEM((levels, SUB, cols), f32),
        pltpu.VMEM((levels, SUB, cols), f32),
        pltpu.VMEM((levels, SUB, cols), f32),
        pltpu.VMEM((levels, SUB, cols), f32),
        pltpu.VMEM((rows, cols), f32),
        pltpu.VMEM(ext, f32),
        pltpu.VMEM((rows, LANE), f32),
        pltpu.VMEM((LANE, rows), f32),
        pltpu.VMEM((2, SUB, cols), f32),
        pltpu.VMEM((2, SUB, rows), f32),
        pltpu.VMEM((4, SUB, LANE), f32),
        pltpu.VMEM((SUB, LANE), f32),
        pltpu.VMEM((ny * nx - 1, SUB, LANE), f32),
        dma((6,)),
        dma,
        dma((2 * len(AROUND),)),
        dma((2 * len(AROUND),)),
        dma,
        dma,
    ]
    return pl.pallas_call(
        functools.partial(kernel, ny, nx),
        out_shape=(
            jax.ShapeDtypeStruct((levels, rows, cols), f32),
            jax.ShapeDtypeStruct((rows, cols), f32),
        ),
        in_specs=[hbm, hbm, hbm, hbm, smem, hbm, hbm],
        out_specs=(hbm, vmem),
        scratch_shapes=scratch,
        compiler_params=pltpu.CompilerParams(collective_id=0, has_side_effects=True),
    )(tracer, east_speed, north_speed, columns, thickness, surface_flux, helm)


def solution(mesh):
    spec = P(None, "gy", "gx")
    flat = P("gy", "gx")
    return jax.shard_map(
        functools.partial(on_device, mesh.shape["gy"], mesh.shape["gx"]),
        mesh=mesh,
        in_specs=(spec, spec, spec, flat, P(), flat, flat),
        out_specs=(spec, flat),
        check_vma=False,
    )
```

```python
import functools

import jax
import jax.numpy as jnp
from jax import lax
from jax.experimental import pallas as pl
from jax.experimental.pallas import tpu as pltpu
from jax.sharding import PartitionSpec as P

TSTEPS = 2
ITERS = 3
MESH = pl.DeviceIdType.MESH
SUB = 8
LANE = 128
AROUND = ((1, 0), (-1, 0), (0, 1), (0, -1), (1, 1), (1, -1), (-1, 1), (-1, -1))


def roll(array, shift, axis):
    shift = shift % array.shape[axis]
    return pltpu.roll(array, shift, axis) if shift else array


def iota(shape, dim):
    return lax.broadcasted_iota(jnp.int32, shape, dim)


def kernel(
    ny,
    nx,
    tracer_ref,
    east_ref,
    north_ref,
    columns_ref,
    thickness_ref,
    surface_ref,
    helm_ref,
    tracer_out,
    heights_out,
    c_ext,
    e_ext,
    n_ext,
    col_in,
    surf_in,
    flat_ext,
    face_levels,
    pack,
    to_left,
    to_right,
    from_left,
    from_right,
    corner_recv,
    up_send,
    down_send,
    up_recv,
    down_recv,
    forcing,
    start_vec,
    flat_pack,
    edge_pack,
    row_recv,
    edge_recv,
    edge_corner_recv,
    part,
    slots,
    in_sem,
    out_sem,
    send_sem,
    recv_sem,
    sum_send_sem,
    sum_recv_sem,
):
    levels, rows, cols = tracer_ref.shape
    ext_rows, ext_cols = rows + SUB, cols + LANE
    my_y, my_x = lax.axis_index("gy"), lax.axis_index("gx")
    count = ny * nx
    my_id = my_y * nx + my_x

    def place(offset):
        target = lax.rem(my_id + offset, count)
        return (target // nx, lax.rem(target, nx))

    def near(dy, dx):
        return (lax.rem(my_y + dy + ny, ny), lax.rem(my_x + dx + nx, nx))

    loads = [
        pltpu.make_async_copy(columns_ref, col_in, in_sem.at[0]),
        pltpu.make_async_copy(helm_ref, flat_ext.at[1, 0:rows, 0:cols], in_sem.at[1]),
        pltpu.make_async_copy(tracer_ref, c_ext.at[:, 0:rows, 0:cols], in_sem.at[2]),
        pltpu.make_async_copy(east_ref, e_ext.at[:, 0:rows, 0:cols], in_sem.at[3]),
        pltpu.make_async_copy(north_ref, n_ext.at[:, 0:rows, 0:cols], in_sem.at[4]),
        pltpu.make_async_copy(surface_ref, surf_in, in_sem.at[5]),
    ]
    for load in loads:
        load.start()
    barrier = pltpu.get_barrier_semaphore()
    for offset in range(1, count):
        pl.semaphore_signal(barrier, inc=1, device_id=place(offset), device_id_type=MESH)
    for load in loads:
        load.wait()

    fields = (c_ext, e_ext, n_ext)
    flat_ext[0, 0:rows, 0:cols] = col_in[...].astype(jnp.float32)

    lane_full = iota((rows, LANE), 1)
    lane_half = lane_full < LANE // 2
    group = lane_full // 4

    def both_edges(ref, index):
        return jnp.where(lane_half, ref[index, 0:rows, 0:LANE], ref[index, 0:rows, cols - LANE : cols])

    sources = [(fields[f], k, f) for k in range(levels) for f in range(3)]
    sources += [(flat_ext, 0, 3), (flat_ext, 1, 4)]
    packed = jnp.zeros((rows, LANE), jnp.float32)
    for slot, (ref, index, _) in enumerate(sources):
        packed = jnp.where(group == slot, roll(both_edges(ref, index), 4 * slot + 2, 1), packed)
    pack[...] = packed
    turned = packed.T
    sub_rows = iota((SUB, rows), 0) % 4 < 2
    for p in range(to_left.shape[0]):
        one, two = turned[2 * SUB * p :][:SUB], turned[2 * SUB * p + SUB :][:SUB]
        to_right[p] = jnp.where(sub_rows, one, roll(two, 2, 0))
        to_left[p] = jnp.where(sub_rows, roll(two, -2, 0), one)

    sub = iota((SUB, cols), 0)
    for k in range(levels):
        quads = [(ref, k) for ref in fields] + [(flat_ext, min(k, 1))]
        up = jnp.zeros((SUB, cols), jnp.float32)
        down = jnp.zeros((SUB, cols), jnp.float32)
        for f, (ref, index) in enumerate(quads):
            mine = sub // 2 == f
            up = jnp.where(mine, roll(ref[index, rows - SUB : rows, 0:cols], 2 * f + 2, 0), up)
            down = jnp.where(mine, roll(ref[index, 0:SUB, 0:cols], 2 * f, 0), down)
        up_send[k] = up
        down_send[k] = down

    pl.semaphore_wait(barrier, count - 1)

    first_rows, last_rows = pl.ds(0, SUB), pl.ds(rows - SUB, SUB)
    first = [
        (up_send, up_recv),
        (down_send, down_recv),
        (to_right, from_left),
        (to_left, from_right),
        (pack.at[last_rows], corner_recv.at[0]),
        (pack.at[last_rows], corner_recv.at[1]),
        (pack.at[first_rows], corner_recv.at[2]),
        (pack.at[first_rows], corner_recv.at[3]),
    ]

    def exchange(pairs, base):
        copies = []
        for which, (source, target) in enumerate(pairs):
            copies.append(
                pltpu.make_async_remote_copy(
                    src_ref=source,
                    dst_ref=target,
                    send_sem=send_sem.at[base + which],
                    recv_sem=recv_sem.at[base + which],
                    device_id=near(*AROUND[which]),
                    device_id_type=MESH,
                )
            )
        for copy in copies:
            copy.start()
        return copies

    copies = exchange(first, 0)
    for copy in copies:
        copy.wait_recv()

    pieces = []
    for p in range(to_left.shape[0]):
        x, y = from_left[p], from_right[p]
        pieces.append(jnp.where(sub_rows, x, y))
        pieces.append(jnp.where(sub_rows, roll(x, -2, 0), roll(y, 2, 0)))
    spare = LANE - 2 * SUB * to_left.shape[0]
    if spare:
        pieces.append(jnp.zeros((spare, rows), jnp.float32))
    sides = jnp.concatenate(pieces, axis=0).T
    small_right = (iota((SUB, LANE), 1) % 4) >= 2
    small_below = iota((SUB, LANE), 0) < SUB // 2
    south = jnp.where(small_right, corner_recv[1], corner_recv[0])
    north = jnp.where(small_right, corner_recv[3], corner_recv[2])
    corner = jnp.where(small_below, north, south)
    for slot, (ref, index, _) in enumerate(sources):
        ref[index, 0:rows, cols:ext_cols] = roll(sides, -4 * slot - 2, 1)
        ref[index, rows:ext_rows, cols:ext_cols] = roll(corner, -4 * slot - 2, 1)
    for k in range(levels):
        quads = [(ref, k) for ref in fields] + ([(flat_ext, k)] if k < 2 else [])
        for f, (ref, index) in enumerate(quads):
            ref[index, rows:ext_rows, 0:cols] = jnp.where(
                sub < SUB // 2,
                roll(down_recv[k], -2 * f, 0),
                roll(up_recv[k], -2 * f - 2, 0),
            )

    row_ids = iota((SUB, ext_cols), 0)
    beyond = (row_ids >= SUB // 2) & (my_y == 0) | (row_ids < SUB // 2) & (my_y == ny - 1)
    flat_ext[0, rows:ext_rows] = jnp.where(beyond, 0.0, flat_ext[0, rows:ext_rows])

    forcing[...] = surf_in[...]

    depth = flat_ext[0]
    face_levels[0] = jnp.minimum(depth, roll(depth, -1, 1))
    face_levels[1] = jnp.minimum(depth, roll(depth, -1, 0))

    def level(k, carry):
        below = lax.convert_element_type(k, jnp.float32)
        east = jnp.where(face_levels[0] > below, e_ext[k], 0.0)
        nort = jnp.where(face_levels[1] > below, n_ext[k], 0.0)
        current = c_ext[k]
        for _ in range(TSTEPS):
            flux_east = east * jnp.where(east > 0.0, current, roll(current, -1, 1))
            flux_north = nort * jnp.where(nort > 0.0, current, roll(current, -1, 0))
            current = current - (
                flux_east - roll(flux_east, 1, 1) + flux_north - roll(flux_north, 1, 0)
            )
        c_ext[k] = current
        open_here = flat_ext[0, 0:rows, 0:cols] > below
        forcing[...] += jnp.where(open_here, thickness_ref[k] * current[0:rows, 0:cols], 0.0)
        return carry

    lax.fori_loop(0, levels, level, 0)

    out_copy = pltpu.make_async_copy(c_ext.at[:, 0:rows, 0:cols], tracer_out, out_sem)
    out_copy.start()

    diagonal = 6.0 + flat_ext[1, 0:rows, 0:cols]
    wet = jnp.where(flat_ext[0, 0:rows, 0:cols] > 0.0, 1.0, 0.0)
    z0 = forcing[...] / diagonal
    y0 = wet * z0
    start_vec[0:rows, 0:cols] = y0
    edges = jnp.where(lane_half, y0[:, 0:LANE], y0[:, cols - LANE : cols])
    flat_pack[...] = edges
    edge_pack[...] = edges.T
    last_lanes = pl.ds(LANE - SUB, SUB)
    second = [
        (start_vec.at[last_rows, pl.ds(0, cols)], row_recv.at[0]),
        (start_vec.at[first_rows, pl.ds(0, cols)], row_recv.at[1]),
        (edge_pack.at[last_lanes], edge_recv.at[0]),
        (edge_pack.at[first_rows], edge_recv.at[1]),
        (flat_pack.at[last_rows], edge_corner_recv.at[0]),
        (flat_pack.at[last_rows], edge_corner_recv.at[1]),
        (flat_pack.at[first_rows], edge_corner_recv.at[2]),
        (flat_pack.at[first_rows], edge_corner_recv.at[3]),
    ]
    more = exchange(second, len(AROUND))
    for copy in more:
        copy.wait_recv()

    turned = jnp.concatenate(
        [edge_recv[1], jnp.zeros((LANE - 2 * SUB, rows), jnp.float32), edge_recv[0]], axis=0
    )
    lane_small = iota((SUB, LANE), 1) < LANE // 2
    south = jnp.where(lane_small, edge_corner_recv[1], edge_corner_recv[0])
    north = jnp.where(lane_small, edge_corner_recv[3], edge_corner_recv[2])
    for copy in more:
        copy.wait_send()
    start_vec[0:rows, cols:ext_cols] = turned.T
    start_vec[rows:ext_rows, cols:ext_cols] = jnp.where(small_below, north, south)
    start_vec[rows:ext_rows, 0:cols] = jnp.where(sub < SUB // 2, row_recv[1], row_recv[0])
    start_vec[rows:ext_rows] = jnp.where(beyond, 0.0, start_vec[rows:ext_rows])

    scale = jnp.where(flat_ext[0] > 0.0, 1.0 / (6.0 + flat_ext[1]), 0.0)

    def off_diagonal(vector):
        across = roll(vector, 1, 1) + roll(vector, -1, 1)
        mixed = vector + 0.5 * across
        return scale * (across + roll(mixed, 1, 0) + roll(mixed, -1, 0))

    z1_ext = off_diagonal(start_vec[...])
    z2_ext = off_diagonal(z1_ext)
    z3_ext = off_diagonal(z2_ext)
    z1, z2, z3 = (z[0:rows, 0:cols] for z in (z1_ext, z2_ext, z3_ext))

    def partial(values):
        folded = jnp.sum(values, axis=0, keepdims=True)
        return sum(folded[:, i : i + LANE] for i in range(0, cols, LANE))

    d0, d1, d2 = (diagonal * z for z in (z0, z1, z2))
    sums = [partial(v) for v in (d0 * z0, d0 * z1, d1 * z1, d1 * z2, d2 * z2, d2 * z3)]
    folded = jnp.concatenate(sums + [jnp.zeros((SUB - len(sums), LANE), jnp.float32)], axis=0)
    for shift in (64, 32, 16):
        folded = folded + roll(folded, shift, 1)
    own = iota((SUB, LANE), 1) // (LANE // SUB) == iota((SUB, LANE), 0)
    part[...] = jnp.sum(jnp.where(own, folded, 0.0), axis=0, keepdims=True)

    for offset in range(1, count):
        pltpu.make_async_remote_copy(
            src_ref=part,
            dst_ref=slots.at[offset - 1],
            send_sem=sum_send_sem,
            recv_sem=sum_recv_sem,
            device_id=place(offset),
            device_id_type=MESH,
        ).start()
    everything = pltpu.make_async_remote_copy(
        src_ref=slots,
        dst_ref=slots,
        send_sem=sum_send_sem,
        recv_sem=sum_recv_sem,
        device_id=place(1),
        device_id_type=MESH,
    )
    everything.wait_recv()
    total = jnp.sum(slots[...], axis=0) + part[...]
    total = jnp.sum(jnp.where(own, total, 0.0), axis=1, keepdims=True)
    moment = [total[i : i + 1, :] for i in range(2 * ITERS)]

    def inner(a, b):
        return sum(x * y * moment[i + j] for i, x in enumerate(a) for j, y in enumerate(b))

    def ratio(top, bottom):
        good = bottom > 0.0
        return jnp.where(good, top / jnp.where(good, bottom, 1.0), 0.0)

    one, zero = jnp.ones((1, 1), jnp.float32), jnp.zeros((1, 1), jnp.float32)
    scaled, direction, height = [one], [one], [zero] * ITERS
    product_now = moment[0]
    for iteration in range(ITERS):
        low, high = direction + [zero], [zero] + direction
        applied = [a - b for a, b in zip(low, high)]
        step_size = ratio(product_now, inner(direction, applied))
        for i, x in enumerate(direction):
            height[i] = height[i] + step_size * x
        if iteration + 1 < ITERS:
            scaled = [a - step_size * b for a, b in zip(scaled + [zero], applied)]
            product_next = jnp.maximum(inner(scaled, scaled), 0.0)
            factor = ratio(product_next, product_now)
            direction = [a + factor * b for a, b in zip(scaled, low)]
            product_now = product_next
    heights_out[...] = height[0] * z0 + height[1] * z1 + height[2] * z2

    everything.wait_send()
    for copy in copies:
        copy.wait_send()
    out_copy.wait()


def on_device(ny, nx, tracer, east_speed, north_speed, columns, thickness, surface_flux, helm):
    levels, rows, cols = tracer.shape
    ext = (rows + SUB, cols + LANE)
    hbm = pl.BlockSpec(memory_space=pl.ANY)
    vmem = pl.BlockSpec(memory_space=pltpu.VMEM)
    smem = pl.BlockSpec(memory_space=pltpu.SMEM)
    f32 = jnp.float32
    dma = pltpu.SemaphoreType.DMA
    pairs = pl.cdiv(4 * (3 * levels + 2), 2 * SUB)
    scratch = [
        pltpu.VMEM((levels, *ext), f32),
        pltpu.VMEM((levels, *ext), f32),
        pltpu.VMEM((levels, *ext), f32),
        pltpu.VMEM((rows, cols), jnp.int32),
        pltpu.VMEM((rows, cols), f32),
        pltpu.VMEM((2, *ext), f32),
        pltpu.VMEM((2, *ext), f32),
        pltpu.VMEM((rows, LANE), f32),
        *[pltpu.VMEM((pairs, SUB, rows), f32)] * 4,
        pltpu.VMEM((4, SUB, LANE), f32),
        pltpu.VMEM((levels, SUB, cols), f32),
        pltpu.VMEM((levels, SUB, cols), f32),
        pltpu.VMEM((levels, SUB, cols), f32),
        pltpu.VMEM((levels, SUB, cols), f32),
        pltpu.VMEM((rows, cols), f32),
        pltpu.VMEM(ext, f32),
        pltpu.VMEM((rows, LANE), f32),
        pltpu.VMEM((LANE, rows), f32),
        pltpu.VMEM((2, SUB, cols), f32),
        pltpu.VMEM((2, SUB, rows), f32),
        pltpu.VMEM((4, SUB, LANE), f32),
        pltpu.VMEM((1, LANE), f32),
        pltpu.VMEM((ny * nx - 1, 1, LANE), f32),
        dma((6,)),
        dma,
        dma((2 * len(AROUND),)),
        dma((2 * len(AROUND),)),
        dma,
        dma,
    ]
    return pl.pallas_call(
        functools.partial(kernel, ny, nx),
        out_shape=(
            jax.ShapeDtypeStruct((levels, rows, cols), f32),
            jax.ShapeDtypeStruct((rows, cols), f32),
        ),
        in_specs=[hbm, hbm, hbm, hbm, smem, hbm, hbm],
        out_specs=(hbm, vmem),
        scratch_shapes=scratch,
        compiler_params=pltpu.CompilerParams(collective_id=0, has_side_effects=True),
    )(tracer, east_speed, north_speed, columns, thickness, surface_flux, helm)


def solution(mesh):
    spec = P(None, "gy", "gx")
    flat = P("gy", "gx")
    return jax.shard_map(
        functools.partial(on_device, mesh.shape["gy"], mesh.shape["gx"]),
        mesh=mesh,
        in_specs=(spec, spec, spec, flat, P(), flat, flat),
        out_specs=(spec, flat),
        check_vma=False,
    )
```

```python
import functools

import jax
import jax.numpy as jnp
from jax import lax
from jax.experimental import pallas as pl
from jax.experimental.pallas import tpu as pltpu
from jax.sharding import PartitionSpec as P

TSTEPS = 2
ITERS = 3
MESH = pl.DeviceIdType.MESH
SUB = 8
LANE = 128
AROUND = ((1, 0), (-1, 0), (0, 1), (0, -1), (1, 1), (1, -1), (-1, 1), (-1, -1))


def roll(array, shift, axis):
    shift = shift % array.shape[axis]
    return pltpu.roll(array, shift, axis) if shift else array


def iota(shape, dim):
    return lax.broadcasted_iota(jnp.int32, shape, dim)


def kernel(
    ny,
    nx,
    tracer_ref,
    east_ref,
    north_ref,
    columns_ref,
    thickness_ref,
    surface_ref,
    helm_ref,
    tracer_out,
    heights_out,
    c_ext,
    e_ext,
    n_ext,
    col_in,
    surf_in,
    flat_ext,
    face_levels,
    pack,
    to_left,
    to_right,
    from_left,
    from_right,
    corner_recv,
    up_send,
    down_send,
    up_recv,
    down_recv,
    forcing,
    start_vec,
    flat_pack,
    edge_pack,
    row_recv,
    edge_recv,
    edge_corner_recv,
    part,
    slots,
    in_sem,
    out_sem,
    send_sem,
    recv_sem,
    sum_send_sem,
    sum_recv_sem,
):
    levels, rows, cols = tracer_ref.shape
    ext_rows, ext_cols = rows + SUB, cols + LANE
    my_y, my_x = lax.axis_index("gy"), lax.axis_index("gx")
    count = ny * nx
    my_id = my_y * nx + my_x

    def place(offset):
        target = lax.rem(my_id + offset, count)
        return (target // nx, lax.rem(target, nx))

    def near(dy, dx):
        return (lax.rem(my_y + dy + ny, ny), lax.rem(my_x + dx + nx, nx))

    loads = [
        pltpu.make_async_copy(columns_ref, col_in, in_sem.at[0]),
        pltpu.make_async_copy(helm_ref, flat_ext.at[1, 0:rows, 0:cols], in_sem.at[1]),
        pltpu.make_async_copy(tracer_ref, c_ext.at[:, 0:rows, 0:cols], in_sem.at[2]),
        pltpu.make_async_copy(east_ref, e_ext.at[:, 0:rows, 0:cols], in_sem.at[3]),
        pltpu.make_async_copy(north_ref, n_ext.at[:, 0:rows, 0:cols], in_sem.at[4]),
        pltpu.make_async_copy(surface_ref, surf_in, in_sem.at[5]),
    ]
    for load in loads:
        load.start()
    barrier = pltpu.get_barrier_semaphore()
    for offset in range(1, count):
        pl.semaphore_signal(barrier, inc=1, device_id=place(offset), device_id_type=MESH)
    for load in loads:
        load.wait()

    fields = (c_ext, e_ext, n_ext)
    flat_ext[0, 0:rows, 0:cols] = col_in[...].astype(jnp.float32)

    lane_full = iota((rows, LANE), 1)
    lane_half = lane_full < LANE // 2
    group = lane_full // 4

    def both_edges(ref, index):
        return jnp.where(lane_half, ref[index, 0:rows, 0:LANE], ref[index, 0:rows, cols - LANE : cols])

    sources = [(fields[f], k, f) for k in range(levels) for f in range(3)]
    sources += [(flat_ext, 0, 3), (flat_ext, 1, 4)]
    packed = jnp.zeros((rows, LANE), jnp.float32)
    for slot, (ref, index, _) in enumerate(sources):
        packed = jnp.where(group == slot, roll(both_edges(ref, index), 4 * slot + 2, 1), packed)
    pack[...] = packed
    turned = packed.T
    sub_rows = iota((SUB, rows), 0) % 4 < 2
    for p in range(to_left.shape[0]):
        one, two = turned[2 * SUB * p :][:SUB], turned[2 * SUB * p + SUB :][:SUB]
        to_right[p] = jnp.where(sub_rows, one, roll(two, 2, 0))
        to_left[p] = jnp.where(sub_rows, roll(two, -2, 0), one)

    sub = iota((SUB, cols), 0)
    for k in range(levels):
        quads = [(ref, k) for ref in fields] + [(flat_ext, min(k, 1))]
        up = jnp.zeros((SUB, cols), jnp.float32)
        down = jnp.zeros((SUB, cols), jnp.float32)
        for f, (ref, index) in enumerate(quads):
            mine = sub // 2 == f
            up = jnp.where(mine, roll(ref[index, rows - SUB : rows, 0:cols], 2 * f + 2, 0), up)
            down = jnp.where(mine, roll(ref[index, 0:SUB, 0:cols], 2 * f, 0), down)
        up_send[k] = up
        down_send[k] = down

    pl.semaphore_wait(barrier, count - 1)

    first_rows, last_rows = pl.ds(0, SUB), pl.ds(rows - SUB, SUB)
    first = [
        (up_send, up_recv),
        (down_send, down_recv),
        (to_right, from_left),
        (to_left, from_right),
        (pack.at[last_rows], corner_recv.at[0]),
        (pack.at[last_rows], corner_recv.at[1]),
        (pack.at[first_rows], corner_recv.at[2]),
        (pack.at[first_rows], corner_recv.at[3]),
    ]

    def exchange(pairs, base):
        copies = []
        for which, (source, target) in enumerate(pairs):
            copies.append(
                pltpu.make_async_remote_copy(
                    src_ref=source,
                    dst_ref=target,
                    send_sem=send_sem.at[base + which],
                    recv_sem=recv_sem.at[base + which],
                    device_id=near(*AROUND[which]),
                    device_id_type=MESH,
                )
            )
        for copy in reversed(copies):
            copy.start()
        return copies

    copies = exchange(first, 0)
    for copy in copies:
        copy.wait_recv()

    pieces = []
    for p in range(to_left.shape[0]):
        x, y = from_left[p], from_right[p]
        pieces.append(jnp.where(sub_rows, x, y))
        pieces.append(jnp.where(sub_rows, roll(x, -2, 0), roll(y, 2, 0)))
    spare = LANE - 2 * SUB * to_left.shape[0]
    if spare:
        pieces.append(jnp.zeros((spare, rows), jnp.float32))
    sides = jnp.concatenate(pieces, axis=0).T
    small_right = (iota((SUB, LANE), 1) % 4) >= 2
    small_below = iota((SUB, LANE), 0) < SUB // 2
    south = jnp.where(small_right, corner_recv[1], corner_recv[0])
    north = jnp.where(small_right, corner_recv[3], corner_recv[2])
    corner = jnp.where(small_below, north, south)
    for slot, (ref, index, _) in enumerate(sources):
        ref[index, 0:rows, cols:ext_cols] = roll(sides, -4 * slot - 2, 1)
        ref[index, rows:ext_rows, cols:ext_cols] = roll(corner, -4 * slot - 2, 1)
    for k in range(levels):
        quads = [(ref, k) for ref in fields] + ([(flat_ext, k)] if k < 2 else [])
        for f, (ref, index) in enumerate(quads):
            ref[index, rows:ext_rows, 0:cols] = jnp.where(
                sub < SUB // 2,
                roll(down_recv[k], -2 * f, 0),
                roll(up_recv[k], -2 * f - 2, 0),
            )

    row_ids = iota((SUB, ext_cols), 0)
    beyond = (row_ids >= SUB // 2) & (my_y == 0) | (row_ids < SUB // 2) & (my_y == ny - 1)
    flat_ext[0, rows:ext_rows] = jnp.where(beyond, 0.0, flat_ext[0, rows:ext_rows])

    forcing[...] = surf_in[...]

    depth = flat_ext[0]
    face_levels[0] = jnp.minimum(depth, roll(depth, -1, 1))
    face_levels[1] = jnp.minimum(depth, roll(depth, -1, 0))

    def level(k, carry):
        below = lax.convert_element_type(k, jnp.float32)
        east = jnp.where(face_levels[0] > below, e_ext[k], 0.0)
        nort = jnp.where(face_levels[1] > below, n_ext[k], 0.0)
        current = c_ext[k]
        for _ in range(TSTEPS):
            flux_east = east * jnp.where(east > 0.0, current, roll(current, -1, 1))
            flux_north = nort * jnp.where(nort > 0.0, current, roll(current, -1, 0))
            current = current - (
                flux_east - roll(flux_east, 1, 1) + flux_north - roll(flux_north, 1, 0)
            )
        c_ext[k] = current
        open_here = flat_ext[0, 0:rows, 0:cols] > below
        forcing[...] += jnp.where(open_here, thickness_ref[k] * current[0:rows, 0:cols], 0.0)
        return carry

    lax.fori_loop(0, levels, level, 0, unroll=2)

    out_copy = pltpu.make_async_copy(c_ext.at[:, 0:rows, 0:cols], tracer_out, out_sem)
    out_copy.start()

    diagonal = 6.0 + flat_ext[1, 0:rows, 0:cols]
    wet = jnp.where(flat_ext[0, 0:rows, 0:cols] > 0.0, 1.0, 0.0)
    z0 = forcing[...] / diagonal
    y0 = wet * z0
    start_vec[0:rows, 0:cols] = y0
    edges = jnp.where(lane_half, y0[:, 0:LANE], y0[:, cols - LANE : cols])
    flat_pack[...] = edges
    edge_pack[...] = edges.T
    last_lanes = pl.ds(LANE - SUB, SUB)
    second = [
        (start_vec.at[last_rows, pl.ds(0, cols)], row_recv.at[0]),
        (start_vec.at[first_rows, pl.ds(0, cols)], row_recv.at[1]),
        (edge_pack.at[last_lanes], edge_recv.at[0]),
        (edge_pack.at[first_rows], edge_recv.at[1]),
        (flat_pack.at[last_rows], edge_corner_recv.at[0]),
        (flat_pack.at[last_rows], edge_corner_recv.at[1]),
        (flat_pack.at[first_rows], edge_corner_recv.at[2]),
        (flat_pack.at[first_rows], edge_corner_recv.at[3]),
    ]
    more = exchange(second, len(AROUND))
    for copy in more:
        copy.wait_recv()

    turned = jnp.concatenate(
        [edge_recv[1], jnp.zeros((LANE - 2 * SUB, rows), jnp.float32), edge_recv[0]], axis=0
    )
    lane_small = iota((SUB, LANE), 1) < LANE // 2
    south = jnp.where(lane_small, edge_corner_recv[1], edge_corner_recv[0])
    north = jnp.where(lane_small, edge_corner_recv[3], edge_corner_recv[2])
    for copy in more:
        copy.wait_send()
    start_vec[0:rows, cols:ext_cols] = turned.T
    start_vec[rows:ext_rows, cols:ext_cols] = jnp.where(small_below, north, south)
    start_vec[rows:ext_rows, 0:cols] = jnp.where(sub < SUB // 2, row_recv[1], row_recv[0])
    start_vec[rows:ext_rows] = jnp.where(beyond, 0.0, start_vec[rows:ext_rows])

    scale = jnp.where(flat_ext[0] > 0.0, 1.0 / (6.0 + flat_ext[1]), 0.0)

    def off_diagonal(vector):
        across = roll(vector, 1, 1) + roll(vector, -1, 1)
        mixed = vector + 0.5 * across
        return scale * (across + roll(mixed, 1, 0) + roll(mixed, -1, 0))

    z1_ext = off_diagonal(start_vec[...])
    z2_ext = off_diagonal(z1_ext)
    z3_ext = off_diagonal(z2_ext)
    z1, z2, z3 = (z[0:rows, 0:cols] for z in (z1_ext, z2_ext, z3_ext))

    def partial(values):
        folded = jnp.sum(values, axis=0, keepdims=True)
        return sum(folded[:, i : i + LANE] for i in range(0, cols, LANE))

    d0, d1, d2 = (diagonal * z for z in (z0, z1, z2))
    sums = [partial(v) for v in (d0 * z0, d0 * z1, d1 * z1, d1 * z2, d2 * z2, d2 * z3)]
    folded = jnp.concatenate(sums + [jnp.zeros((SUB - len(sums), LANE), jnp.float32)], axis=0)
    for shift in (64, 32, 16):
        folded = folded + roll(folded, shift, 1)
    own = iota((SUB, LANE), 1) // (LANE // SUB) == iota((SUB, LANE), 0)
    part[...] = jnp.sum(jnp.where(own, folded, 0.0), axis=0, keepdims=True)

    for offset in range(1, count):
        pltpu.make_async_remote_copy(
            src_ref=part,
            dst_ref=slots.at[offset - 1],
            send_sem=sum_send_sem,
            recv_sem=sum_recv_sem,
            device_id=place(offset),
            device_id_type=MESH,
        ).start()
    everything = pltpu.make_async_remote_copy(
        src_ref=slots,
        dst_ref=slots,
        send_sem=sum_send_sem,
        recv_sem=sum_recv_sem,
        device_id=place(1),
        device_id_type=MESH,
    )
    everything.wait_recv()
    total = jnp.sum(slots[...], axis=0) + part[...]
    total = jnp.sum(jnp.where(own, total, 0.0), axis=1, keepdims=True)
    moment = [total[i : i + 1, :] for i in range(2 * ITERS)]

    def inner(a, b):
        return sum(x * y * moment[i + j] for i, x in enumerate(a) for j, y in enumerate(b))

    def ratio(top, bottom):
        good = bottom > 0.0
        return jnp.where(good, top / jnp.where(good, bottom, 1.0), 0.0)

    one, zero = jnp.ones((1, 1), jnp.float32), jnp.zeros((1, 1), jnp.float32)
    scaled, direction, height = [one], [one], [zero] * ITERS
    product_now = moment[0]
    for iteration in range(ITERS):
        low, high = direction + [zero], [zero] + direction
        applied = [a - b for a, b in zip(low, high)]
        step_size = ratio(product_now, inner(direction, applied))
        for i, x in enumerate(direction):
            height[i] = height[i] + step_size * x
        if iteration + 1 < ITERS:
            scaled = [a - step_size * b for a, b in zip(scaled + [zero], applied)]
            product_next = jnp.maximum(inner(scaled, scaled), 0.0)
            factor = ratio(product_next, product_now)
            direction = [a + factor * b for a, b in zip(scaled, low)]
            product_now = product_next
    heights_out[...] = height[0] * z0 + height[1] * z1 + height[2] * z2

    everything.wait_send()
    for copy in copies:
        copy.wait_send()
    out_copy.wait()


def hand_on(tracer_ref, heights_ref, tracer_out, heights_out, tracer_held, heights_held, load, save):
    levels = tracer_ref.shape[0]
    stages = [(tracer_ref.at[k], tracer_held.at[k], tracer_out.at[k]) for k in range(levels)]
    stages.append((heights_ref, heights_held, heights_out))
    loads = [pltpu.make_async_copy(a, b, load.at[i]) for i, (a, b, _) in enumerate(stages)]
    saves = [pltpu.make_async_copy(b, c, save.at[i]) for i, (_, b, c) in enumerate(stages)]
    for copy in loads:
        copy.start()
    for copy, onward in zip(loads, saves):
        copy.wait()
        onward.start()
    for onward in saves:
        onward.wait()


def on_device(ny, nx, tracer, east_speed, north_speed, columns, thickness, surface_flux, helm):
    levels, rows, cols = tracer.shape
    ext = (rows + SUB, cols + LANE)
    hbm = pl.BlockSpec(memory_space=pl.ANY)
    vmem = pl.BlockSpec(memory_space=pltpu.VMEM)
    smem = pl.BlockSpec(memory_space=pltpu.SMEM)
    f32 = jnp.float32
    dma = pltpu.SemaphoreType.DMA
    pairs = pl.cdiv(4 * (3 * levels + 2), 2 * SUB)
    scratch = [
        pltpu.VMEM((levels, *ext), f32),
        pltpu.VMEM((levels, *ext), f32),
        pltpu.VMEM((levels, *ext), f32),
        pltpu.VMEM((rows, cols), jnp.int32),
        pltpu.VMEM((rows, cols), f32),
        pltpu.VMEM((2, *ext), f32),
        pltpu.VMEM((2, *ext), f32),
        pltpu.VMEM((rows, LANE), f32),
        *[pltpu.VMEM((pairs, SUB, rows), f32)] * 4,
        pltpu.VMEM((4, SUB, LANE), f32),
        pltpu.VMEM((levels, SUB, cols), f32),
        pltpu.VMEM((levels, SUB, cols), f32),
        pltpu.VMEM((levels, SUB, cols), f32),
        pltpu.VMEM((levels, SUB, cols), f32),
        pltpu.VMEM((rows, cols), f32),
        pltpu.VMEM(ext, f32),
        pltpu.VMEM((rows, LANE), f32),
        pltpu.VMEM((LANE, rows), f32),
        pltpu.VMEM((2, SUB, cols), f32),
        pltpu.VMEM((2, SUB, rows), f32),
        pltpu.VMEM((4, SUB, LANE), f32),
        pltpu.VMEM((1, LANE), f32),
        pltpu.VMEM((ny * nx - 1, 1, LANE), f32),
        dma((6,)),
        dma,
        dma((2 * len(AROUND),)),
        dma((2 * len(AROUND),)),
        dma,
        dma,
    ]
    results = pl.pallas_call(
        functools.partial(kernel, ny, nx),
        out_shape=(
            jax.ShapeDtypeStruct((levels, rows, cols), f32),
            jax.ShapeDtypeStruct((rows, cols), f32),
        ),
        in_specs=[hbm, hbm, hbm, hbm, smem, hbm, hbm],
        out_specs=(hbm, vmem),
        scratch_shapes=scratch,
        compiler_params=pltpu.CompilerParams(collective_id=0, has_side_effects=True),
    )(tracer, east_speed, north_speed, columns, thickness, surface_flux, helm)
    return pl.pallas_call(
        hand_on,
        out_shape=tuple(jax.ShapeDtypeStruct(r.shape, f32) for r in results),
        in_specs=[hbm, hbm],
        out_specs=(hbm, hbm),
        scratch_shapes=[
            pltpu.VMEM((levels, rows, cols), f32),
            pltpu.VMEM((rows, cols), f32),
            dma((levels + 1,)),
            dma((levels + 1,)),
        ],
    )(*results)


def solution(mesh):
    spec = P(None, "gy", "gx")
    flat = P("gy", "gx")
    return jax.shard_map(
        functools.partial(on_device, mesh.shape["gy"], mesh.shape["gx"]),
        mesh=mesh,
        in_specs=(spec, spec, spec, flat, P(), flat, flat),
        out_specs=(spec, flat),
        check_vma=False,
    )
```
